256 devices in a mesh: pop: 16 (over y, z_hi, core), col: 16 (over z_lo, x).
Axes of the slice: x: 4, y: 4, z: 8 (z_hi: 2, z_lo: 4; z = z_hi * 4 + z_lo), core: 2. Of those that a mesh axis runs over, the one named last changes fastest.
Arguments:
- tokens: bfloat16 [14336, 4096], P('pop'), may hold values from -6 to 6
- weight: bfloat16 [4096, 16384], P(None, ('col', 'pop')), may hold values from -0.09375 to 0.09375
- old_left: bfloat16 [1792, 4, 4096], P('pop', None, 'col'), may hold values from -6 to 6
- old_right: bfloat16 [1792, 4, 16384], P('pop', None, 'col'), may hold values from -6 to 6
- selected: int32 [16, 8], P('pop'), may hold values from 0 to 111, as said below
- shaping: float32 [16, 8], P('pop'), may hold values from -3 to 3
- new_left: bfloat16 [1792, 4, 4096], P('pop', None, 'col'), may hold values from -6 to 6
- new_right: bfloat16 [1792, 4, 16384], P('pop', None, 'col'), may hold values from -6 to 6
Outputs:
- updated: bfloat16 [4096, 16384], P(None, ('col', 'pop'))
- activations: bfloat16 [14336, 16384], P('pop', 'col')
The draws below stay inside these ranges and needn't reach their ends.
Inputs may be any that keep to these rules, and one draw needn't show every extreme that they name: `selected`: each row names 8 different members of its group.
All inputs are finite; a program needn't handle non-finite values.
Results may differ from the reference program's by a relative error of at most 0.0055.
Values may be sent and summed in bfloat16 or wider, within the bound.
A program may use at most 128 MiB of HBM per device.

```python
import math
import jax
import jax.numpy as jnp
from jax import lax

D = 4096
H = 16384
RANK = 4
TOK_MEM = 8
MEM_DEV = 112
SEL_DEV = 8
MEMBERS = 1792
TOKENS = 14336
N_POP = 16


def draw_selected(key, part):
    scores = jax.random.randint(key, (N_POP, MEM_DEV), 0, 2 ** 20, dtype=jnp.int32)
    scores = scores * MEM_DEV + jnp.arange(MEM_DEV, dtype=jnp.int32)[None, :]
    order = jnp.argsort(scores, axis=1, stable=True)
    return order[:, :SEL_DEV].astype(jnp.int32)


def block_levels(key, dims, shards, least, largest):
    gain, own = 1.0, jax.random.fold_in(key, 6)
    for position, blocks in shards:
        heights = jnp.exp(jax.random.uniform(jax.random.fold_in(own, position), (blocks,), jnp.float32, least / len(shards), largest / len(shards)))
        gain = gain * jnp.repeat(heights, dims[position] // blocks).reshape([-1 if axis == position else 1 for axis in range(len(dims))])
    return gain


def scatter_about(own_key, extent, spread, bound, cuts=(), held_as=jnp.bfloat16):
    array = spread * jax.random.normal(own_key, extent, jnp.float32)
    if cuts:
        array = array * block_levels(own_key, extent, cuts, -0.22, 0.18)
    return jnp.clip(array, -bound, bound).astype(held_as)


def setup_inputs(seed: int = 0) -> dict:
    splits = jax.random.split(jax.random.key(seed), 9)
    return {
        "tokens": scatter_about(splits[0], (TOKENS, D), 1.0, 6.0, ((0, 16),)),
        "weight": scatter_about(splits[1], (D, H), D ** -0.5, 0.09375, ((1, 256),)),
        "old_left": scatter_about(splits[2], (MEMBERS, RANK, D), 1.0, 6.0, ((0, 16), (2, 16))),
        "old_right": scatter_about(splits[3], (MEMBERS, RANK, H), 1.0, 6.0, ((0, 16), (2, 16))),
        "selected": draw_selected(jax.random.fold_in(splits[8], 71), 0),
        "shaping": scatter_about(splits[5], (N_POP, SEL_DEV), 0.5, 3.0, ((0, 16),), jnp.float32),
        "new_left": scatter_about(splits[6], (MEMBERS, RANK, D), 1.0, 6.0, ((0, 16), (2, 16))),
        "new_right": scatter_about(splits[7], (MEMBERS, RANK, H), 1.0, 6.0, ((0, 16), (2, 16))),
    }


noise_scale = 0.5

def reference(tokens, weight, old_left, old_right, selected, shaping, new_left, new_right):
    members = (jnp.arange(N_POP, dtype=jnp.int32)[:, None] * MEM_DEV + selected.astype(jnp.int32)).reshape(-1)
    factor = 1.0 / math.sqrt(D * RANK * SEL_DEV * N_POP)
    weights_here = shaping.reshape(-1) * factor
    scaled_left = (old_left[members].astype(jnp.float32) * weights_here[:, None, None]).astype(jnp.bfloat16)
    chosen_right = old_right[members]
    delta = jnp.dot(scaled_left.reshape(-1, D).T, chosen_right.reshape(-1, H), preferred_element_type=jnp.float32)
    updated = (weight.astype(jnp.float32) + delta).astype(jnp.bfloat16)
    side_scale = noise_scale / math.sqrt(D * RANK)

    def group_forward(args):
        rows, lefts, rights = args
        base = jnp.dot(rows, updated, preferred_element_type=jnp.float32)
        per_member = rows.reshape(MEM_DEV, TOK_MEM, D).astype(jnp.float32)
        proj = jnp.einsum('mtd,mrd->mtr', per_member, lefts.astype(jnp.float32), precision=lax.Precision.HIGHEST).astype(jnp.bfloat16)
        side = jnp.einsum('mtr,mrh->mth', proj.astype(jnp.float32), rights.astype(jnp.float32), precision=lax.Precision.HIGHEST).reshape(MEM_DEV * TOK_MEM, H)
        pre = base + side_scale * side
        return (jnp.maximum(pre, 0.0) ** 2).astype(jnp.bfloat16)
    outputs = lax.map(group_forward, (tokens.reshape(N_POP, MEM_DEV * TOK_MEM, D), new_left.reshape(N_POP, MEM_DEV, RANK, D), new_right.reshape(N_POP, MEM_DEV, RANK, H)))
    return (updated, outputs.reshape(TOKENS, H))
```

```python
import functools
import math

import jax
import jax.numpy as jnp
from jax import lax
from jax.experimental import pallas as pl
from jax.experimental.pallas import tpu as pltpu
from jax.sharding import PartitionSpec as P

MESH = pl.DeviceIdType.MESH
F32, BF16 = jnp.float32, jnp.bfloat16

D = 4096
RANK = 4
ROWS = 896
COLS = 1024
OWN = 64
MEM = 112
SEL = 8
SLAB = 256
CHUNKS = 8
LEN = D // CHUNKS
RCH = CHUNKS
NCH = CHUNKS + 1
noise_scale = 0.5
FACTOR = 1.0 / math.sqrt(D * RANK * SEL * 16)
SIDE = noise_scale / math.sqrt(D * RANK)


def nt(a, b):
    return lax.dot_general(a, b, (((1,), (1,)), ((), ())), preferred_element_type=F32)


def nn(a, b):
    return lax.dot_general(a, b, (((1,), (0,)), ((), ())), preferred_element_type=F32)


def kernel(
    tok_h, w_h, oldl_h, oldr_h, sel, shp, newl_h, newr_h,
    upd_h, act_h,
    tok, wall, rall, lall, trw, trr, oldl, oldr, newl, newr, nl, nr,
    acc, tacc, tb, cx, cz, rt, upd, outv,
    ld, st, ssw, sly, slz, slx, sls, spx,
    rp, rm, r2, tz, rz, dd, ly, lzp, lzm, lxp, lxm, lx2, dl, px,
):
    pop, col = lax.axis_index("pop"), lax.axis_index("col")
    y, zh, core = pop // 4, (pop // 2) % 2, pop % 2
    zlo, x = col // 4, col % 4
    z = zh * 4 + zlo

    def dev(y_, z_, core_, x_):
        return (y_ * 4 + (z_ // 4) * 2 + core_, (z_ % 4) * 4 + x_)

    yp, ym, yo = (y + 1) % 4, (y + 3) % 4, (y + 2) % 4
    xp, xm, xo = (x + 1) % 4, (x + 3) % 4, (x + 2) % 4
    Yp, Ym, Yo = dev(yp, z, core, x), dev(ym, z, core, x), dev(yo, z, core, x)
    Xp, Xm, Xo = dev(y, z, core, xp), dev(y, z, core, xm), dev(y, z, core, xo)

    def zdev(step):
        return dev(y, (z + step + 8) % 8, core, x)

    Zp1, Zm1, Zp2, Zm2 = zdev(1), zdev(-1), zdev(2), zdev(-2)
    Sib = dev(y, z, 1 - core, x)
    Zl = [dev(y, zh * 4 + (zlo + j) % 4, core, x) for j in (1, 2, 3)]

    def send(src, dst, ssem, rsem, to):
        pltpu.make_async_remote_copy(
            src_ref=src, dst_ref=dst, send_sem=ssem, recv_sem=rsem,
            device_id=to, device_id_type=MESH,
        ).start()

    def arrived(dst, rsem):
        pltpu.make_async_remote_copy(
            src_ref=dst, dst_ref=dst, send_sem=ssw.at[0], recv_sem=rsem,
            device_id=Sib, device_id_type=MESH,
        ).wait_recv()

    def sent(src, ssem):
        pltpu.make_async_remote_copy(
            src_ref=src, dst_ref=src, send_sem=ssem, recv_sem=rp.at[0, 0],
            device_id=Sib, device_id_type=MESH,
        ).wait_send()

    def piece(zh_, y_, k):
        if k == RCH:
            return rall.at[pl.ds(pl.multiple_of(((zh_ * 2 + core) * 4 + y_) * 32, 32), 32), :]
        return wall.at[zh_, pl.ds(pl.multiple_of((y_ * 2 + core) * OWN, OWN), OWN), k * LEN:(k + 1) * LEN]

    def transit(k):
        return trr if k == RCH else trw.at[k]

    def lpiece(z_, x_):
        c_ = (z_ % 4) * 4 + x_
        return lall.at[c_, pl.ds(pl.multiple_of(((z_ // 4) * 2 + core) * 128, 128), 128), :]

    mine = wall.at[zh, pl.ds(pl.multiple_of((y * 2 + core) * OWN, OWN), OWN), :]
    loads = [
        pltpu.make_async_copy(s, d, ld.at[i])
        for i, (s, d) in enumerate((
            (w_h, mine), (oldl_h, oldl), (oldr_h, oldr), (newl_h, newl), (newr_h, newr), (tok_h, tok),
        ))
    ]
    for cp in loads:
        cp.start()

    barrier = pltpu.get_barrier_semaphore()
    partners = [Yp, Ym, Yo, Xp, Xm, Xo, Zp1, Zm1, Zp2, Zm2, Sib] + Zl
    for to in partners:
        pl.semaphore_signal(barrier, inc=1, device_id=to, device_id_type=MESH)

    def rows_of(ref, ids, scales=None):
        parts = [ref[i].astype(F32) for i in ids]
        if scales is not None:
            parts = [p * s for p, s in zip(parts, scales)]
        return jnp.concatenate(parts, axis=0).astype(BF16)

    ids = [sel[0, j] for j in range(SEL)]
    loads[1].wait()
    lrow = pl.multiple_of((zh * 2 + core) * 128 + y * 32, 32)
    lall[col, pl.ds(lrow, 32), :] = rows_of(oldl, ids, [shp[0, j] * F32(FACTOR) for j in range(SEL)])
    loads[2].wait()
    v = rows_of(oldr, ids)
    rrow = pl.multiple_of(((zh * 2 + core) * 4 + y) * 32, 32)
    for b in range(8):
        h_, y_ = b % 2, b // 2
        rall[pl.ds(rrow, 32), h_ * 512 + y_ * 128:h_ * 512 + (y_ + 1) * 128] = v[:, b * 128:(b + 1) * 128]
    loads[0].wait()
    pl.semaphore_wait(barrier, len(partners))

    def start_left():
        src = lall.at[col, pl.ds(lrow, 32), :]
        for j, to in enumerate((Yp, Ym, Yo)):
            send(src, src, sly.at[j], ly.at[j], to)

    def own_y(k):
        src = piece(zh, y, k)
        send(src, src, ssw.at[k], rp.at[0, k], Yp)
        send(src, src, ssw.at[k], rm.at[0, k], Ym)
        send(src, src, ssw.at[k], dd.at[0, k], Sib)

    def own_z(k):
        send(piece(zh, y, k), transit(k), ssw.at[k], tz.at[k], Zp2 if k % 2 == 0 else Zm2)

    def pass_z(k):
        arrived(transit(k), tz.at[k])
        step = -2 if k % 2 == 0 else 2
        from_zh = ((z + step + 8) % 8) // 4
        send(transit(k), piece(from_zh, y, k), ssw.at[k], rz.at[k], Zp2 if k % 2 == 0 else Zm2)

    def other_y(k):
        src = piece(1 - zh, y, k)
        arrived(src, rz.at[k])
        send(src, src, ssw.at[k], rp.at[1, k], Yp)
        send(src, src, ssw.at[k], rm.at[1, k], Ym)
        send(src, src, ssw.at[k], dd.at[1, k], Sib)

    def got_p(s, k):
        h_ = zh if s == 0 else 1 - zh
        src = piece(h_, ym, k)
        arrived(src, rp.at[s, k])
        if k % 2 == 0:
            send(src, src, ssw.at[k], r2.at[s, k], Yp)
        send(src, src, ssw.at[k], dd.at[s, k], Sib)

    def got_m(s, k):
        h_ = zh if s == 0 else 1 - zh
        src = piece(h_, yp, k)
        arrived(src, rm.at[s, k])
        if k % 2 == 1:
            send(src, src, ssw.at[k], r2.at[s, k], Ym)
        send(src, src, ssw.at[k], dd.at[s, k], Sib)

    def got_2(s, k):
        h_ = zh if s == 0 else 1 - zh
        src = piece(h_, yo, k)
        arrived(src, r2.at[s, k])
        send(src, src, ssw.at[k], dd.at[s, k], Sib)

    def got_all(s, k):
        if k == RCH:
            arrived(rall.at[0:128, :], dd.at[s, k])
        else:
            h_ = zh if s == 0 else 1 - zh
            arrived(wall.at[h_, 0:256, k * LEN:(k + 1) * LEN], dd.at[s, k])

    def z_of(i):
        return z if i == 0 else ((z + 8 - i) % 8 if i <= 4 else (z + i - 4) % 8)

    def left_out(i):
        src = lpiece(z_of(i), x)
        send(src, src, slx, lxp.at[i], Xp)
        send(src, src, slx, lxm.at[i], Xm)
        send(src, src, sls, dl.at[(z_of(i) % 4) * 4 + x], Sib)

    def left_own():
        for j, y_ in enumerate((ym, yp, yo)):
            arrived(lall.at[col, pl.ds(pl.multiple_of((zh * 2 + core) * 128 + y_ * 32, 32), 32), :], ly.at[j])
        src = lpiece(z, x)
        send(src, src, slz.at[0], lzp.at[0], Zp1)
        send(src, src, slz.at[1], lzm.at[0], Zm1)
        left_out(0)

    def left_p(d):
        src = lpiece(z_of(d), x)
        arrived(src, lzp.at[d - 1])
        if d < 4:
            send(src, src, slz.at[1 + d], lzp.at[d], Zp1)
        left_out(d)

    def left_m(d):
        src = lpiece(z_of(4 + d), x)
        arrived(src, lzm.at[d - 1])
        if d < 3:
            send(src, src, slz.at[4 + d], lzm.at[d], Zm1)
        left_out(4 + d)

    def left_x(which, i):
        x_, sem = {"p": (xm, lxp), "m": (xp, lxm), "2": (xo, lx2)}[which]
        src = lpiece(z_of(i), x_)
        arrived(src, sem.at[i])
        if which == "p" and i % 2 == 0:
            send(src, src, slx, lx2.at[i], Xp)
        if which == "m" and i % 2 == 1:
            send(src, src, slx, lx2.at[i], Xm)
        send(src, src, sls, dl.at[(z_of(i) % 4) * 4 + x_], Sib)

    def build_new():
        nl[448:512, :] = jnp.zeros((64, SLAB), BF16)
        for h_ in range(2):
            nr[h_, 448:512, :] = jnp.zeros((64, 512), BF16)
        loads[3].wait()
        loads[4].wait()

        def body(i, _):
            at = pl.ds(pl.multiple_of(i * 32, 32), 32)
            nl[at, :] = rows_of(newl, [i * 8 + j for j in range(8)])
            v = rows_of(newr, [i * 8 + j for j in range(8)])
            for b in range(8):
                nr[b % 2, at, (b // 2) * 128:(b // 2 + 1) * 128] = v[:, b * 128:(b + 1) * 128]
            return 0

        lax.fori_loop(0, MEM // 8, body, 0)

    def own_member(n):
        r = lax.broadcasted_iota(jnp.int32, (n, 128), 0)
        c = lax.broadcasted_iota(jnp.int32, (n, 128), 1)
        return (r >> 3) == (c >> 2)

    def proj_part():
        loads[5].wait()
        lanes = pl.ds(pl.multiple_of(col * SLAB, SLAB), SLAB)
        for g in range(4):
            n = 256 if g < 3 else 128
            part = nt(tok[256 * g:256 * g + n, lanes], nl[128 * g:128 * (g + 1), :])
            part = jnp.where(own_member(n), part, 0.0)
            cx[x, :, 128 * g:128 * (g + 1)] = part.reshape(n // 8, 8, 128).sum(axis=0)
        src = cx.at[x]
        for j, to in enumerate((Xp, Xm, Xo)):
            send(src, src, spx.at[j], px.at[0], to)

    def proj_x():
        arrived(cx.at[0:3], px.at[0])
        cz[zlo] = (cx[0] + cx[1]) + (cx[2] + cx[3])
        src = cz.at[zlo]
        for j, to in enumerate(Zl):
            send(src, src, spx.at[3 + j], px.at[1], to)

    def proj_z():
        arrived(cz.at[0:3], px.at[1])
        proj = ((cz[0] + cz[1]) + (cz[2] + cz[3])).astype(BF16).astype(F32)
        for g in range(4):
            n = 256 if g < 3 else 128
            wide = jnp.broadcast_to(proj[:, 128 * g:128 * (g + 1)][None], (n // 8, 8, 128)).reshape(n, 128)
            wide = jnp.where(own_member(n), wide, 0.0).astype(BF16)
            for h_ in range(2):
                acc[h_, 256 * g:256 * g + n, :] = nn(wide, nr[h_, 128 * g:128 * (g + 1), :]) * SIDE

    def main_dot(s, k):
        h_ = zh if s == 0 else 1 - zh

        def body(n, _):
            at = pl.ds(pl.multiple_of(n * 256, 256), 256)
            acc[h_, :, at] += nt(tok[:, k * LEN:(k + 1) * LEN], wall[h_, at, k * LEN:(k + 1) * LEN])
            return 0

        lax.fori_loop(0, 2, body, 0)

    def t_dot(x_, first):
        for zlo_ in range(4):
            c = zlo_ * 4 + x_
            arrived(lall.at[c, 0:256, :], dl.at[c])

        def body(zlo_, _):
            c = zlo_ * 4 + x_
            part = nt(tok[:, pl.ds(pl.multiple_of(c * SLAB, SLAB), SLAB)], lall[c])
            tacc[...] += part
            return 0

        if first:
            tacc[...] = jnp.zeros_like(tacc)
        lax.fori_loop(0, 4, body, 0)

    def make_rt():
        base = pl.multiple_of(zh * 512 + y * 128, 128)
        rt[...] = rall[:, pl.ds(base, 128)].astype(F32).T.astype(BF16)

    def update(x_):
        def body(zlo_, _):
            c = zlo_ * 4 + x_
            at = pl.ds(pl.multiple_of(c * SLAB, SLAB), SLAB)
            own = wall[zh, pl.ds(pl.multiple_of((y * 2 + core) * OWN, OWN), OWN), at]
            delta = nn(rt[pl.ds(pl.multiple_of(core * OWN, OWN), OWN), :], lall[c])
            upd[:, at] = (own.astype(F32) + delta).astype(BF16)
            return 0

        lax.fori_loop(0, 4, body, 0)

    def t_right():
        tb[...] = tacc[...].astype(BF16)

        def body(i, _):
            h_, at = i // 2, pl.ds(pl.multiple_of((i % 2) * 256, 256), 256)
            acc[h_, :, at] += nn(tb[...], rall[:, pl.ds(pl.multiple_of(i * 256, 256), 256)])
            return 0

        lax.fori_loop(0, 4, body, 0)

    def out_copy(s, y_):
        h_ = zh if s == 0 else 1 - zh
        at = pl.ds(pl.multiple_of((2 * y_ + h_) * 128, 128), 128)
        return pltpu.make_async_copy(outv.at[:, at], act_h.at[:, at], st.at[s * 4 + y_])

    def finish(s):
        h_ = zh if s == 0 else 1 - zh
        for y_ in range(4):
            at = pl.ds(pl.multiple_of((2 * y_ + h_) * 128, 128), 128)
            pre = jnp.maximum(acc[h_, :, y_ * 128:(y_ + 1) * 128], 0.0)
            outv[:, at] = (pre * pre).astype(BF16)
            out_copy(s, y_).start()

    def store_update():
        pltpu.make_async_copy(upd, upd_h, st.at[8]).start()

    order = [RCH] + list(range(CHUNKS))
    events = [(0.0, start_left)]
    for i, k in enumerate(order):
        events.append((0.1 + 0.001 * i, functools.partial(own_y, k)))
        events.append((0.1005 + 0.001 * i if i < 4 else 3.0 + 2.0 * (i // 2), functools.partial(own_z, k)))
        for s, base in ((0, 3.0), (1, 0.0)):
            t = 3.2 + 1.5 * i if s == 0 else 20.5 + 2.0 * i
            events.append((t, functools.partial(got_p, s, k)))
            events.append((t + 0.001, functools.partial(got_m, s, k)))
            t2 = 15.0 + 0.7 * i if s == 0 else 25.0 + 1.8 * i
            events.append((t2, functools.partial(got_2, s, k)))
            events.append((t2 + 2.0, functools.partial(got_all, s, k)))
            if k != RCH:
                events.append((t2 + 2.01, functools.partial(main_dot, s, k)))
        pair = i // 2
        events.append((5.0 + 4.0 * pair, functools.partial(pass_z, k)))
        events.append((9.5 + 4.5 * pair, functools.partial(other_y, k)))
    events += [
        (1.0, build_new), (2.0, proj_part), (3.5, left_own), (6.0, proj_x), (9.0, proj_z),
    ]
    for d in range(1, 5):
        events.append((3.5 + 4.0 * d, functools.partial(left_p, d)))
        if d < 4:
            events.append((3.51 + 4.0 * d, functools.partial(left_m, d)))
    for i in range(8):
        step = 0 if i == 0 else (i if i <= 4 else i - 4)
        t = 7.5 + 4.0 * step
        events.append((t, functools.partial(left_x, "p", i)))
        events.append((t + 0.001, functools.partial(left_x, "m", i)))
        events.append((t + 4.0, functools.partial(left_x, "2", i)))
    events += [
        (28.1, functools.partial(t_dot, x, True)),
        (28.2, functools.partial(t_dot, xm, False)),
        (28.3, functools.partial(t_dot, xp, False)),
        (30.1, functools.partial(t_dot, xo, False)),
        (30.2, t_right),
        (32.9, make_rt),
        (33.0, functools.partial(update, x)),
        (33.1, functools.partial(update, xm)),
        (33.2, functools.partial(update, xp)),
        (33.3, functools.partial(update, xo)),
        (33.4, store_update),
        (33.5, functools.partial(finish, 0)),
        (90.0, functools.partial(finish, 1)),
    ]
    for _, event in sorted(events, key=lambda e: e[0]):
        event()

    for k in range(NCH):
        sent(wall.at[:, :, 0:LEN], ssw.at[k])
    for j in range(3):
        sent(lall.at[0, 0:32, :], sly.at[j])
    for j in range(7):
        sent(lall.at[0, 0:128, :], slz.at[j])
    sent(lall.at[0:6], slx)
    sent(lall.at[0:8], sls)
    for j in range(6):
        sent(cx.at[0], spx.at[j])
    for s in range(2):
        for y_ in range(4):
            out_copy(s, y_).wait()
    pltpu.make_async_copy(upd, upd_h, st.at[8]).wait()


def local(tokens, weight, old_left, old_right, selected, shaping, new_left, new_right):
    dma = pltpu.SemaphoreType.DMA
    anywhere = pl.BlockSpec(memory_space=pl.ANY)
    scalars = pl.BlockSpec(memory_space=pltpu.SMEM)
    upd, act = pl.pallas_call(
        kernel,
        out_shape=(
            jax.ShapeDtypeStruct((OWN, D), BF16),
            jax.ShapeDtypeStruct((ROWS, COLS), BF16),
        ),
        in_specs=[anywhere] * 4 + [scalars] * 2 + [anywhere] * 2,
        out_specs=(anywhere, anywhere),
        scratch_shapes=[
            pltpu.VMEM((ROWS, D), BF16),
            pltpu.VMEM((2, 512, D), BF16),
            pltpu.VMEM((512, COLS), BF16),
            pltpu.VMEM((16, 512, SLAB), BF16),
            pltpu.VMEM((CHUNKS, OWN, LEN), BF16),
            pltpu.VMEM((32, COLS), BF16),
            pltpu.VMEM((MEM, RANK, SLAB), BF16),
            pltpu.VMEM((MEM, RANK, COLS), BF16),
            pltpu.VMEM((MEM, RANK, SLAB), BF16),
            pltpu.VMEM((MEM, RANK, COLS), BF16),
            pltpu.VMEM((512, SLAB), BF16),
            pltpu.VMEM((2, 512, 512), BF16),
            pltpu.VMEM((2, ROWS, 512), F32),
            pltpu.VMEM((ROWS, 512), F32),
            pltpu.VMEM((ROWS, 512), BF16),
            pltpu.VMEM((4, 8, 512), F32),
            pltpu.VMEM((4, 8, 512), F32),
            pltpu.VMEM((128, 512), BF16),
            pltpu.VMEM((OWN, D), BF16),
            pltpu.VMEM((ROWS, COLS), BF16),
            dma((6,)), dma((9,)), dma((NCH,)), dma((3,)), dma((7,)), dma(()), dma(()), dma((6,)),
            dma((2, NCH)), dma((2, NCH)), dma((2, NCH)), dma((NCH,)), dma((NCH,)), dma((2, NCH)),
            dma((3,)), dma((4,)), dma((3,)), dma((8,)), dma((8,)), dma((8,)), dma((16,)), dma((2,)),
        ],
        compiler_params=pltpu.CompilerParams(
            collective_id=0, has_side_effects=True, vmem_limit_bytes=56 * 1024 * 1024
        ),
        name="gather_and_project",
    )(tokens, weight.T, old_left, old_right, selected, shaping, new_left, new_right)
    return (upd.T, act)


def solution(mesh):
    placed = (
        P("pop", None),
        P(None, ("col", "pop")),
        P("pop", None, "col"),
        P("pop", None, "col"),
        P("pop", None),
        P("pop", None),
        P("pop", None, "col"),
        P("pop", None, "col"),
    )
    return jax.shard_map(
        local,
        mesh=mesh,
        in_specs=placed,
        out_specs=(P(None, ("col", "pop")), P("pop", "col")),
        check_vma=False,
    )
```

```python
import functools
import math

import jax
import jax.numpy as jnp
from jax import lax
from jax.experimental import pallas as pl
from jax.experimental.pallas import tpu as pltpu
from jax.sharding import PartitionSpec as P

MESH = pl.DeviceIdType.MESH
F32, BF16 = jnp.float32, jnp.bfloat16

D = 4096
RANK = 4
ROWS = 896
COLS = 1024
OWN = 64
MEM = 112
SEL = 8
SLAB = 256
CHUNKS = 8
LEN = D // CHUNKS
RCH = CHUNKS
NCH = CHUNKS + 1
noise_scale = 0.5
ORDER = (
    ("start_left",), ("own_y", 0), ("own_y", 1), ("own_y", 2), ("own_y", 3), ("pick_right",), ("own_y", 8),
    ("own_y", 4), ("own_y", 5), ("own_y", 6), ("own_y", 7), ("build_new",), ("proj_part",), ("own_z", 0),
    ("own_z", 1), ("own_z", 2), ("own_z", 3), ("got_m", 0, 0), ("left_own",), ("proj_x",), ("got_p", 0, 0),
    ("got_m", 0, 1), ("got_p", 0, 1), ("own_z", 8), ("own_z", 4), ("got_m", 0, 2), ("pass_z", 0), ("pass_z", 1),
    ("got_p", 0, 2), ("got_m", 0, 3), ("got_p", 0, 3), ("got_m", 0, 8), ("pass_z", 2), ("pass_z", 3),
    ("left_x", "m", 0), ("left_x", "p", 0), ("left_p", 1), ("left_m", 1), ("got_p", 0, 8), ("proj_z",),
    ("got_p", 0, 4), ("got_m", 0, 4), ("got_m", 0, 5), ("got_p", 0, 5), ("got_m", 0, 6), ("pass_z", 4),
    ("pass_z", 8), ("got_p", 0, 6), ("got_m", 0, 7), ("left_x", "2", 0), ("left_x", "m", 1), ("got_p", 0, 7),
    ("got_2", 0, 1), ("left_x", "p", 1), ("other_y", 0), ("other_y", 1), ("left_x", "m", 5), ("got_2", 0, 0),
    ("got_2", 0, 3), ("left_x", "p", 5), ("got_2", 0, 2), ("own_z", 5), ("own_z", 6), ("got_2", 0, 8),
    ("other_y", 2), ("other_y", 3), ("got_2", 0, 4), ("left_p", 2), ("left_m", 2), ("got_2", 0, 5),
    ("main_dot", 0, 0, 1), ("left_x", "2", 1), ("got_2", 0, 6), ("main_dot", 0, 2, 3), ("left_x", "2", 5),
    ("got_2", 0, 7), ("own_z", 7), ("got_p", 1, 0), ("got_r", 0), ("got_m", 1, 0), ("other_y", 4), ("other_y", 8),
    ("main_dot", 0, 4, 5), ("got_m", 1, 1), ("got_p", 1, 1), ("got_p", 1, 2), ("left_x", "m", 2), ("left_x", "p", 2),
    ("got_m", 1, 2), ("main_dot", 0, 6, 7), ("left_m", 3), ("left_p", 3), ("left_x", "m", 6), ("left_x", "p", 6),
    ("got_m", 1, 3), ("pass_z", 5), ("pass_z", 6), ("got_p", 1, 3), ("got_2", 1, 0), ("got_m", 1, 4),
    ("got_p", 1, 4), ("got_m", 1, 8), ("pass_z", 7), ("left_x", "2", 2), ("got_p", 1, 8), ("got_2", 1, 1),
    ("got_2", 1, 2), ("left_x", "m", 7), ("left_p", 4), ("left_x", "p", 7), ("got_2", 1, 3), ("left_x", "m", 3),
    ("left_x", "p", 3), ("main_dot", 1, 0, 1), ("other_y", 5), ("left_x", "2", 6), ("got_2", 1, 8), ("got_2", 1, 4),
    ("t_dot", 0), ("other_y", 6), ("main_dot", 1, 2, 3), ("other_y", 7), ("left_x", "2", 7), ("left_x", "p", 4),
    ("left_x", "m", 4), ("got_r", 1), ("make_rt",), ("update", 0), ("left_x", "2", 3), ("got_m", 1, 5),
    ("got_p", 1, 5), ("t_dot", 1), ("got_m", 1, 6), ("got_p", 1, 6), ("t_dot", 2), ("left_x", "2", 4),
    ("got_m", 1, 7), ("got_p", 1, 7), ("update", 1), ("update", 2), ("got_2", 1, 5), ("t_dot", 3), ("got_2", 1, 6),
    ("t_right", 0), ("t_right", 1), ("got_2", 1, 7), ("update", 3), ("main_dot", 1, 4, 5), ("finish", 0),
    ("main_dot", 1, 6), ("main_dot", 1, 7), ("finish", 1),
)
FACTOR = 1.0 / math.sqrt(D * RANK * SEL * 16)
SIDE = noise_scale / math.sqrt(D * RANK)


def going_up(k):
    return k % 2 == 0 and k != RCH


def nt(a, b):
    return lax.dot_general(a, b, (((1,), (1,)), ((), ())), preferred_element_type=F32)


def nn(a, b):
    return lax.dot_general(a, b, (((1,), (0,)), ((), ())), preferred_element_type=F32)


def kernel(
    tok_h, w_h, oldl_h, oldr_h, sel, shp, newl_h, newr_h,
    upd, outv,
    tok, wall, rall, lall, trw, trr, oldl, oldr, newl, newr, nl, nr,
    acc, tacc, tb, cx, cz, rt,
    ld, ssw, sly, slz, slx, sls, spx,
    rp, rm, r2, tz, rz, dd, ly, lzp, lzm, lxp, lxm, lx2, dl, px,
):
    pop, col = lax.axis_index("pop"), lax.axis_index("col")
    y, zh, core = pop // 4, (pop // 2) % 2, pop % 2
    zlo, x = col // 4, col % 4
    z = zh * 4 + zlo

    def dev(y_, z_, core_, x_):
        return (y_ * 4 + (z_ // 4) * 2 + core_, (z_ % 4) * 4 + x_)

    yp, ym, yo = (y + 1) % 4, (y + 3) % 4, (y + 2) % 4
    xp, xm, xo = (x + 1) % 4, (x + 3) % 4, (x + 2) % 4
    Yp, Ym, Yo = dev(yp, z, core, x), dev(ym, z, core, x), dev(yo, z, core, x)
    Xp, Xm, Xo = dev(y, z, core, xp), dev(y, z, core, xm), dev(y, z, core, xo)

    def zdev(step):
        return dev(y, (z + step + 8) % 8, core, x)

    Zp1, Zm1, Zp2, Zm2 = zdev(1), zdev(-1), zdev(2), zdev(-2)
    Sib = dev(y, z, 1 - core, x)
    Zl = [dev(y, zh * 4 + (zlo + j) % 4, core, x) for j in (1, 2, 3)]

    def send(src, dst, ssem, rsem, to):
        pltpu.make_async_remote_copy(
            src_ref=src, dst_ref=dst, send_sem=ssem, recv_sem=rsem,
            device_id=to, device_id_type=MESH,
        ).start()

    def arrived(dst, rsem):
        pltpu.make_async_remote_copy(
            src_ref=dst, dst_ref=dst, send_sem=ssw.at[0], recv_sem=rsem,
            device_id=Sib, device_id_type=MESH,
        ).wait_recv()

    def sent(src, ssem):
        pltpu.make_async_remote_copy(
            src_ref=src, dst_ref=src, send_sem=ssem, recv_sem=rp.at[0, 0],
            device_id=Sib, device_id_type=MESH,
        ).wait_send()

    def piece(zh_, y_, k):
        if k == RCH:
            return rall.at[pl.ds(pl.multiple_of(((zh_ * 2 + core) * 4 + y_) * 32, 32), 32), :]
        return wall.at[zh_, pl.ds(pl.multiple_of((y_ * 2 + core) * OWN, OWN), OWN), k * LEN:(k + 1) * LEN]

    def transit(k):
        return trr if k == RCH else trw.at[k]

    def lpiece(z_, x_):
        c_ = (z_ % 4) * 4 + x_
        return lall.at[c_, pl.ds(pl.multiple_of(((z_ // 4) * 2 + core) * 128, 128), 128), :]

    mine = wall.at[zh, pl.ds(pl.multiple_of((y * 2 + core) * OWN, OWN), OWN), :]
    loads = [
        pltpu.make_async_copy(s, d, ld.at[i])
        for i, (s, d) in enumerate((
            (w_h, mine), (oldl_h, oldl), (oldr_h, oldr), (newl_h, newl), (newr_h, newr), (tok_h, tok),
        ))
    ]
    for i in (1, 0, 2, 5, 3, 4):
        loads[i].start()

    barrier = pltpu.get_barrier_semaphore()
    partners = [Yp, Ym, Yo, Xp, Xm, Xo, Zp1, Zm1, Zp2, Zm2, Sib] + Zl
    for to in partners:
        pl.semaphore_signal(barrier, inc=1, device_id=to, device_id_type=MESH)

    def rows_of(ref, ids, scales=None):
        parts = [ref[i].astype(F32) for i in ids]
        if scales is not None:
            parts = [p * s for p, s in zip(parts, scales)]
        return jnp.concatenate(parts, axis=0).astype(BF16)

    ids = [sel[0, j] for j in range(SEL)]
    loads[1].wait()
    lrow = pl.multiple_of((zh * 2 + core) * 128 + y * 32, 32)
    lall[col, pl.ds(lrow, 32), :] = rows_of(oldl, ids, [shp[0, j] * F32(FACTOR) for j in range(SEL)])
    loads[0].wait()
    pl.semaphore_wait(barrier, len(partners))

    def start_left():
        src = lall.at[col, pl.ds(lrow, 32), :]
        for j, to in enumerate((Yp, Ym, Yo)):
            send(src, src, sly.at[j], ly.at[j], to)

    def own_y(k):
        src = piece(zh, y, k)
        send(src, src, ssw.at[k], rp.at[0, k], Yp)
        send(src, src, ssw.at[k], rm.at[0, k], Ym)
        send(src, src, ssw.at[k], dd.at[0, k], Sib)

    def own_z(k):
        send(piece(zh, y, k), transit(k), ssw.at[k], tz.at[k], Zp2 if going_up(k) else Zm2)

    def pass_z(k):
        arrived(transit(k), tz.at[k])
        step = -2 if going_up(k) else 2
        from_zh = ((z + step + 8) % 8) // 4
        send(transit(k), piece(from_zh, y, k), ssw.at[k], rz.at[k], Zp2 if going_up(k) else Zm2)

    def other_y(k):
        src = piece(1 - zh, y, k)
        arrived(src, rz.at[k])
        send(src, src, ssw.at[k], rp.at[1, k], Yp)
        send(src, src, ssw.at[k], rm.at[1, k], Ym)
        send(src, src, ssw.at[k], dd.at[1, k], Sib)

    def got_p(s, k):
        h_ = zh if s == 0 else 1 - zh
        src = piece(h_, ym, k)
        arrived(src, rp.at[s, k])
        if going_up(k):
            send(src, src, ssw.at[k], r2.at[s, k], Yp)
        send(src, src, ssw.at[k], dd.at[s, k], Sib)

    def got_m(s, k):
        h_ = zh if s == 0 else 1 - zh
        src = piece(h_, yp, k)
        arrived(src, rm.at[s, k])
        if not going_up(k):
            send(src, src, ssw.at[k], r2.at[s, k], Ym)
        send(src, src, ssw.at[k], dd.at[s, k], Sib)

    def got_2(s, k):
        h_ = zh if s == 0 else 1 - zh
        src = piece(h_, yo, k)
        arrived(src, r2.at[s, k])
        send(src, src, ssw.at[k], dd.at[s, k], Sib)

    def got_r(s):
        arrived(rall.at[0:128, :], dd.at[s, RCH])

    def z_of(i):
        return z if i == 0 else ((z + 8 - i) % 8 if i <= 4 else (z + i - 4) % 8)

    def left_out(i):
        src = lpiece(z_of(i), x)
        send(src, src, slx, lxp.at[i], Xp)
        send(src, src, slx, lxm.at[i], Xm)
        send(src, src, sls, dl.at[(z_of(i) % 4) * 4 + x], Sib)

    def left_own():
        for j, y_ in enumerate((ym, yp, yo)):
            arrived(lall.at[col, pl.ds(pl.multiple_of((zh * 2 + core) * 128 + y_ * 32, 32), 32), :], ly.at[j])
        src = lpiece(z, x)
        send(src, src, slz.at[0], lzp.at[0], Zp1)
        send(src, src, slz.at[1], lzm.at[0], Zm1)
        left_out(0)

    def left_p(d):
        src = lpiece(z_of(d), x)
        arrived(src, lzp.at[d - 1])
        if d < 4:
            send(src, src, slz.at[1 + d], lzp.at[d], Zp1)
        left_out(d)

    def left_m(d):
        src = lpiece(z_of(4 + d), x)
        arrived(src, lzm.at[d - 1])
        if d < 3:
            send(src, src, slz.at[4 + d], lzm.at[d], Zm1)
        left_out(4 + d)

    def left_x(which, i):
        x_, sem = {"p": (xm, lxp), "m": (xp, lxm), "2": (xo, lx2)}[which]
        src = lpiece(z_of(i), x_)
        arrived(src, sem.at[i])
        if which == "p" and i % 2 == 0:
            send(src, src, slx, lx2.at[i], Xp)
        if which == "m" and i % 2 == 1:
            send(src, src, slx, lx2.at[i], Xm)
        send(src, src, sls, dl.at[(z_of(i) % 4) * 4 + x_], Sib)

    def pick_right():
        loads[2].wait()
        v = rows_of(oldr, ids)
        rrow = pl.multiple_of(((zh * 2 + core) * 4 + y) * 32, 32)
        for b in range(8):
            h_, y_ = b % 2, b // 2
            rall[pl.ds(rrow, 32), h_ * 512 + y_ * 128:h_ * 512 + (y_ + 1) * 128] = v[:, b * 128:(b + 1) * 128]

    def build_new():
        nl[448:512, :] = jnp.zeros((64, SLAB), BF16)
        for h_ in range(2):
            nr[h_, 448:512, :] = jnp.zeros((64, 512), BF16)
        loads[3].wait()
        loads[4].wait()

        def body(i, _):
            at = pl.ds(pl.multiple_of(i * 32, 32), 32)
            nl[at, :] = rows_of(newl, [i * 8 + j for j in range(8)])
            v = rows_of(newr, [i * 8 + j for j in range(8)])
            for b in range(8):
                nr[b % 2, at, (b // 2) * 128:(b // 2 + 1) * 128] = v[:, b * 128:(b + 1) * 128]
            return 0

        lax.fori_loop(0, MEM // 8, body, 0)

    def own_member(n):
        r = lax.broadcasted_iota(jnp.int32, (n, 128), 0)
        c = lax.broadcasted_iota(jnp.int32, (n, 128), 1)
        return (r >> 3) == (c >> 2)

    def proj_part():
        loads[5].wait()
        lanes = pl.ds(pl.multiple_of(col * SLAB, SLAB), SLAB)
        for g in range(4):
            n = 256 if g < 3 else 128
            part = nt(tok[256 * g:256 * g + n, lanes], nl[128 * g:128 * (g + 1), :])
            part = jnp.where(own_member(n), part, 0.0)
            cx[x, :, 128 * g:128 * (g + 1)] = part.reshape(n // 8, 8, 128).sum(axis=0)
        src = cx.at[x]
        for j, to in enumerate((Xp, Xm, Xo)):
            send(src, src, spx.at[j], px.at[0], to)

    def proj_x():
        arrived(cx.at[0:3], px.at[0])
        cz[zlo] = (cx[0] + cx[1]) + (cx[2] + cx[3])
        src = cz.at[zlo]
        for j, to in enumerate(Zl):
            send(src, src, spx.at[3 + j], px.at[1], to)

    def proj_z():
        arrived(cz.at[0:3], px.at[1])
        proj = ((cz[0] + cz[1]) + (cz[2] + cz[3])).astype(BF16).astype(F32)
        for g in range(4):
            n = 256 if g < 3 else 128
            wide = jnp.broadcast_to(proj[:, 128 * g:128 * (g + 1)][None], (n // 8, 8, 128)).reshape(n, 128)
            wide = jnp.where(own_member(n), wide, 0.0).astype(BF16)
            for h_ in range(2):
                acc[h_, 256 * g:256 * g + n, :] = nn(wide, nr[h_, 128 * g:128 * (g + 1), :]) * SIDE

    def main_dot(s, *ks):
        h_ = zh if s == 0 else 1 - zh
        for k in ks:
            arrived(wall.at[h_, 0:256, k * LEN:(k + 1) * LEN], dd.at[s, k])
        deep = slice(ks[0] * LEN, (ks[-1] + 1) * LEN)
        for n in range(2):
            at = slice(n * 256, (n + 1) * 256)
            acc[h_, :, at] += nt(tok[:, deep], wall[h_, at, deep])

    xs = (x, xm, xp, xo)

    def slab(c):
        return pl.ds(pl.multiple_of(c * SLAB, SLAB), SLAB)

    def t_dot(j):
        cs = [zlo_ * 4 + xs[j] for zlo_ in range(4)]
        for c in cs:
            arrived(lall.at[c, 0:256, :], dl.at[c])
        part = sum(nt(tok[:, slab(c)], lall[c]) for c in cs)
        tacc[...] = part if j == 0 else tacc[...] + part

    def make_rt():
        base = pl.multiple_of(zh * 512 + y * 128, 128)
        rt[...] = rall[:, pl.ds(base, 128)].astype(F32).T.astype(BF16)

    def update(j):
        left = rt[pl.ds(pl.multiple_of(core * OWN, OWN), OWN), :]
        for c in [zlo_ * 4 + xs[j] for zlo_ in range(4)]:
            own = wall[zh, pl.ds(pl.multiple_of((y * 2 + core) * OWN, OWN), OWN), slab(c)]
            upd[:, slab(c)] = (own.astype(F32) + nn(left, lall[c])).astype(BF16)

    def t_right(h_):
        if h_ == 0:
            tb[...] = tacc[...].astype(BF16)
        for n in range(2):
            at = slice(n * 256, (n + 1) * 256)
            acc[h_, :, at] += nn(tb[...], rall[:, h_ * 512 + n * 256:h_ * 512 + (n + 1) * 256])

    def finish(s):
        h_ = zh if s == 0 else 1 - zh
        for y_ in range(4):
            at = pl.ds(pl.multiple_of((2 * y_ + h_) * 128, 128), 128)
            pre = jnp.maximum(acc[h_, :, y_ * 128:(y_ + 1) * 128], 0.0)
            outv[:, at] = (pre * pre).astype(BF16)

    steps = {f.__name__: f for f in (
        start_left, own_y, own_z, pass_z, other_y, got_p, got_m, got_2, got_r, left_own, left_p, left_m, left_x,
        pick_right, build_new, proj_part, proj_x, proj_z, main_dot, t_dot, make_rt, update, t_right, finish,
    )}
    for name, *rest in ORDER:
        steps[name](*rest)

    for k in range(NCH):
        sent(wall.at[:, :, 0:LEN], ssw.at[k])
    for j in range(3):
        sent(lall.at[0, 0:32, :], sly.at[j])
    for j in range(7):
        sent(lall.at[0, 0:128, :], slz.at[j])
    sent(lall.at[0:6], slx)
    sent(lall.at[0:8], sls)
    for j in range(6):
        sent(cx.at[0], spx.at[j])


def local(tokens, weight, old_left, old_right, selected, shaping, new_left, new_right):
    dma = pltpu.SemaphoreType.DMA
    anywhere = pl.BlockSpec(memory_space=pl.ANY)
    scalars = pl.BlockSpec(memory_space=pltpu.SMEM)
    upd, act = pl.pallas_call(
        kernel,
        out_shape=(pltpu.VMEM((OWN, D), BF16), pltpu.VMEM((ROWS, COLS), BF16)),
        in_specs=[anywhere] * 4 + [scalars] * 2 + [anywhere] * 2,
        out_specs=(pl.BlockSpec(memory_space=pltpu.VMEM),) * 2,
        scratch_shapes=[
            pltpu.VMEM((ROWS, D), BF16),
            pltpu.VMEM((2, 512, D), BF16),
            pltpu.VMEM((512, COLS), BF16),
            pltpu.VMEM((16, 512, SLAB), BF16),
            pltpu.VMEM((CHUNKS, OWN, LEN), BF16),
            pltpu.VMEM((32, COLS), BF16),
            pltpu.VMEM((MEM, RANK, SLAB), BF16),
            pltpu.VMEM((MEM, RANK, COLS), BF16),
            pltpu.VMEM((MEM, RANK, SLAB), BF16),
            pltpu.VMEM((MEM, RANK, COLS), BF16),
            pltpu.VMEM((512, SLAB), BF16),
            pltpu.VMEM((2, 512, 512), BF16),
            pltpu.VMEM((2, ROWS, 512), F32),
            pltpu.VMEM((ROWS, 512), F32),
            pltpu.VMEM((ROWS, 512), BF16),
            pltpu.VMEM((4, 8, 512), F32),
            pltpu.VMEM((4, 8, 512), F32),
            pltpu.VMEM((128, 512), BF16),
            dma((6,)), dma((NCH,)), dma((3,)), dma((7,)), dma(()), dma(()), dma((6,)),
            dma((2, NCH)), dma((2, NCH)), dma((2, NCH)), dma((NCH,)), dma((NCH,)), dma((2, NCH)),
            dma((3,)), dma((4,)), dma((3,)), dma((8,)), dma((8,)), dma((8,)), dma((16,)), dma((2,)),
        ],
        compiler_params=pltpu.CompilerParams(
            collective_id=0, has_side_effects=True, vmem_limit_bytes=56 * 1024 * 1024
        ),
        name="gather_and_project",
    )(tokens, weight.T, old_left, old_right, selected, shaping, new_left, new_right)
    return (upd.T, act)


def solution(mesh):
    placed = (
        P("pop", None),
        P(None, ("col", "pop")),
        P("pop", None, "col"),
        P("pop", None, "col"),
        P("pop", None),
        P("pop", None),
        P("pop", None, "col"),
        P("pop", None, "col"),
    )
    return jax.shard_map(
        local,
        mesh=mesh,
        in_specs=placed,
        out_specs=(P(None, ("col", "pop")), P("pop", "col")),
        check_vma=False,
    )
```

```python
import functools
import math

import jax
import jax.numpy as jnp
from jax import lax
from jax.experimental import pallas as pl
from jax.experimental.pallas import tpu as pltpu
from jax.sharding import PartitionSpec as P

MESH = pl.DeviceIdType.MESH
F32, BF16 = jnp.float32, jnp.bfloat16

D = 4096
RANK = 4
ROWS = 896
COLS = 1024
OWN = 64
MEM = 112
SEL = 8
SLAB = 256
CHUNKS = 8
LEN = D // CHUNKS
RCH = CHUNKS
NCH = CHUNKS + 1
noise_scale = 0.5
ORDER = (
    ("start_left",), ("own_y", 0), ("own_z", 0), ("own_y", 1), ("own_z", 1), ("own_y", 2), ("own_y", 3),
    ("pick_right",), ("own_y", 8), ("own_y", 4), ("build_new",), ("proj_part",), ("own_z", 2), ("own_z", 3),
    ("own_y", 5), ("own_z", 8), ("own_z", 4), ("own_y", 6), ("own_z", 5), ("own_z", 6), ("own_y", 7), ("pass_z", 0),
    ("left_own",), ("got_m", 0, 0), ("proj_x",), ("got_p", 0, 0), ("got_m", 0, 1), ("got_p", 0, 1), ("got_m", 0, 2),
    ("got_p", 0, 2), ("pass_z", 1), ("got_m", 0, 3), ("got_p", 0, 3), ("left_x", "m", 0), ("left_x", "p", 0),
    ("got_m", 0, 8), ("got_p", 0, 8), ("got_m", 0, 4), ("got_p", 0, 4), ("left_z", 6), ("pass_z", 2), ("left_z", 5),
    ("got_m", 0, 5), ("got_p", 0, 5), ("pass_z", 3), ("other_y", 0), ("got_m", 0, 6), ("left_x", "2", 0),
    ("got_p", 0, 6), ("got_m", 0, 7), ("got_p", 0, 7), ("left_z", 2), ("left_z", 1), ("left_x", "m", 6),
    ("left_x", "p", 6), ("got_2", 0, 1), ("got_2", 0, 0), ("pass_z", 8), ("left_x", "m", 5), ("left_x", "p", 5),
    ("got_2", 0, 3), ("left_z", 7), ("got_2", 0, 2), ("other_y", 1), ("got_2", 0, 8), ("proj_z",), ("got_2", 0, 4),
    ("pass_z", 4), ("main_dot", 0, 0, 1), ("got_2", 0, 5), ("left_x", "m", 2), ("left_x", "p", 2), ("got_p", 1, 0),
    ("main_dot", 0, 2, 3), ("left_z", 3), ("left_x", "m", 1), ("own_z", 7), ("left_x", "p", 1), ("got_m", 1, 0),
    ("got_2", 0, 6), ("other_y", 2), ("got_r", 0), ("pass_z", 5), ("left_x", "2", 5), ("left_x", "2", 6),
    ("got_2", 0, 7), ("got_p", 1, 1), ("other_y", 3), ("main_dot", 0, 4, 5), ("left_x", "m", 7), ("left_x", "p", 7),
    ("got_m", 1, 1), ("pass_z", 6), ("left_z", 4), ("left_x", "2", 2), ("got_2", 1, 0), ("main_dot", 0, 6, 7),
    ("left_x", "m", 3), ("got_m", 1, 2), ("left_x", "p", 3), ("got_p", 1, 2), ("pass_z", 7), ("other_y", 8),
    ("t_dot", 0), ("left_x", "2", 1), ("got_m", 1, 3), ("got_p", 1, 3), ("left_x", "2", 7), ("got_2", 1, 1),
    ("other_y", 4), ("left_x", "p", 4), ("left_x", "m", 4), ("got_2", 1, 2), ("left_x", "2", 3), ("got_m", 1, 8),
    ("main_dot", 1, 0, 1), ("other_y", 5), ("got_p", 1, 8), ("t_dot", 1), ("other_y", 6), ("got_2", 1, 3),
    ("t_dot", 2), ("left_x", "2", 4), ("got_m", 1, 4), ("got_p", 1, 4), ("other_y", 7), ("got_2", 1, 8),
    ("main_dot", 1, 2, 3), ("got_p", 1, 5), ("t_dot", 3), ("got_m", 1, 5), ("got_p", 1, 6), ("got_m", 1, 6),
    ("got_r", 1), ("make_rt",), ("t_right", 0), ("t_right", 1), ("got_2", 1, 4), ("update", 0), ("update", 1),
    ("got_m", 1, 7), ("update", 2), ("update", 3), ("got_p", 1, 7), ("finish", 0), ("got_2", 1, 5), ("got_2", 1, 6),
    ("main_dot", 1, 4, 5), ("got_2", 1, 7), ("main_dot", 1, 6), ("main_dot", 1, 7), ("finish", 1),
)
FACTOR = 1.0 / math.sqrt(D * RANK * SEL * 16)
SIDE = noise_scale / math.sqrt(D * RANK)


def batch(s, k):
    if s == 0:
        return k // 2
    return 5 + (k // 2 if k < 6 else k - 3)


def going_up(k):
    return k % 2 == 0 and k != RCH


def nt(a, b):
    return lax.dot_general(a, b, (((1,), (1,)), ((), ())), preferred_element_type=F32)


def nn(a, b):
    return lax.dot_general(a, b, (((1,), (0,)), ((), ())), preferred_element_type=F32)


def kernel(
    tok_h, w_h, oldl_h, oldr_h, sel, shp, newl_h, newr_h,
    upd, outv,
    tok, wall, rall, lall, trw, trr, oldl, oldr, newl, newr, nl, nr,
    acc, tacc, tb, cx, cz, rt,
    ld, ssw, sly, slz, slx, sls, spx,
    rp, rm, r2, tz, rz, dd, ly, lz, lxp, lxm, lx2, dl, px,
):
    pop, col = lax.axis_index("pop"), lax.axis_index("col")
    y, zh, core = pop // 4, (pop // 2) % 2, pop % 2
    zlo, x = col // 4, col % 4
    z = zh * 4 + zlo

    def dev(y_, z_, core_, x_):
        return (y_ * 4 + (z_ // 4) * 2 + core_, (z_ % 4) * 4 + x_)

    yp, ym, yo = (y + 1) % 4, (y + 3) % 4, (y + 2) % 4
    xp, xm, xo = (x + 1) % 4, (x + 3) % 4, (x + 2) % 4
    Yp, Ym, Yo = dev(yp, z, core, x), dev(ym, z, core, x), dev(yo, z, core, x)
    Xp, Xm, Xo = dev(y, z, core, xp), dev(y, z, core, xm), dev(y, z, core, xo)

    def zdev(step):
        return dev(y, (z + step + 8) % 8, core, x)

    Zp1, Zm1, Zp2, Zm2, Zp3, Zm3 = [zdev(step) for step in (1, -1, 2, -2, 3, -3)]
    Sib = dev(y, z, 1 - core, x)
    Zl = [dev(y, zh * 4 + (zlo + j) % 4, core, x) for j in (1, 2, 3)]

    def send(src, dst, ssem, rsem, to):
        pltpu.make_async_remote_copy(
            src_ref=src, dst_ref=dst, send_sem=ssem, recv_sem=rsem,
            device_id=to, device_id_type=MESH,
        ).start()

    def arrived(dst, rsem):
        pltpu.make_async_remote_copy(
            src_ref=dst, dst_ref=dst, send_sem=ssw.at[0], recv_sem=rsem,
            device_id=Sib, device_id_type=MESH,
        ).wait_recv()

    def sent(src, ssem):
        pltpu.make_async_remote_copy(
            src_ref=src, dst_ref=src, send_sem=ssem, recv_sem=rp.at[0, 0],
            device_id=Sib, device_id_type=MESH,
        ).wait_send()

    def piece(zh_, y_, k):
        if k == RCH:
            return rall.at[pl.ds(pl.multiple_of(((zh_ * 2 + core) * 4 + y_) * 32, 32), 32), :]
        return wall.at[zh_, pl.ds(pl.multiple_of((y_ * 2 + core) * OWN, OWN), OWN), k * LEN:(k + 1) * LEN]

    def transit(k):
        return trr if k == RCH else trw.at[k]

    def lpiece(z_, x_):
        c_ = (z_ % 4) * 4 + x_
        return lall.at[c_, pl.ds(pl.multiple_of(((z_ // 4) * 2 + core) * 128, 128), 128), :]

    mine = wall.at[zh, pl.ds(pl.multiple_of((y * 2 + core) * OWN, OWN), OWN), :]
    loads = [
        pltpu.make_async_copy(s, d, ld.at[i])
        for i, (s, d) in enumerate((
            (w_h, mine), (oldl_h, oldl), (oldr_h, oldr), (newl_h, newl), (newr_h, newr), (tok_h, tok),
        ))
    ]
    for i in (1, 0, 2, 5, 3, 4):
        loads[i].start()

    barrier = pltpu.get_barrier_semaphore()
    partners = [Yp, Ym, Yo, Xp, Xm, Xo, Zp1, Zm1, Zp2, Zm2, Zp3, Zm3, Sib] + Zl
    for to in partners:
        pl.semaphore_signal(barrier, inc=1, device_id=to, device_id_type=MESH)

    def rows_of(ref, ids, scales=None):
        parts = [ref[i].astype(F32) for i in ids]
        if scales is not None:
            parts = [p * s for p, s in zip(parts, scales)]
        return jnp.concatenate(parts, axis=0).astype(BF16)

    ids = [sel[0, j] for j in range(SEL)]
    loads[1].wait()
    lrow = pl.multiple_of((zh * 2 + core) * 128 + y * 32, 32)
    lall[col, pl.ds(lrow, 32), :] = rows_of(oldl, ids, [shp[0, j] * F32(FACTOR) for j in range(SEL)])
    loads[0].wait()
    pl.semaphore_wait(barrier, len(partners))

    def start_left():
        src = lall.at[col, pl.ds(lrow, 32), :]
        for j, to in enumerate((Yp, Ym, Yo)):
            send(src, src, sly, ly, to)

    def own_y(k):
        src = piece(zh, y, k)
        send(src, src, ssw.at[k // 4], rp.at[0, k], Yp)
        send(src, src, ssw.at[k // 4], rm.at[0, k], Ym)
        send(src, src, ssw.at[k // 4], dd.at[batch(0, k)], Sib)

    def own_z(k):
        send(piece(zh, y, k), transit(k), ssw.at[k // 4], tz.at[k], Zp1 if going_up(k) else Zm1)

    def pass_z(k):
        arrived(transit(k), tz.at[k])
        from_zh = ((z + (7 if going_up(k) else 1)) % 8) // 4
        send(transit(k), piece(from_zh, y, k), ssw.at[k // 4], rz.at[k], Zp3 if going_up(k) else Zm3)

    def other_y(k):
        src = piece(1 - zh, y, k)
        arrived(src, rz.at[k])
        send(src, src, ssw.at[k // 4], rp.at[1, k], Yp)
        send(src, src, ssw.at[k // 4], rm.at[1, k], Ym)
        send(src, src, ssw.at[k // 4], dd.at[batch(1, k)], Sib)

    def got_p(s, k):
        h_ = zh if s == 0 else 1 - zh
        src = piece(h_, ym, k)
        arrived(src, rp.at[s, k])
        if going_up(k):
            send(src, src, ssw.at[k // 4], r2.at[s, k], Yp)
        send(src, src, ssw.at[k // 4], dd.at[batch(s, k)], Sib)

    def got_m(s, k):
        h_ = zh if s == 0 else 1 - zh
        src = piece(h_, yp, k)
        arrived(src, rm.at[s, k])
        if not going_up(k):
            send(src, src, ssw.at[k // 4], r2.at[s, k], Ym)
        send(src, src, ssw.at[k // 4], dd.at[batch(s, k)], Sib)

    def got_2(s, k):
        h_ = zh if s == 0 else 1 - zh
        src = piece(h_, yo, k)
        arrived(src, r2.at[s, k])
        send(src, src, ssw.at[k // 4], dd.at[batch(s, k)], Sib)

    def got_r(s):
        arrived(rall.at[0:128, :], dd.at[batch(s, RCH)])

    def z_of(i):
        return z if i == 0 else ((z + 8 - i) % 8 if i <= 4 else (z + i - 4) % 8)

    def left_out(i):
        src = lpiece(z_of(i), x)
        send(src, src, slx, lxp.at[i], Xp)
        send(src, src, slx, lxm.at[i], Xm)
        send(src, src, sls, dl.at[0], Sib)

    def left_own():
        arrived(lall.at[0, 0:96, :], ly)
        src = lpiece(z, x)
        for i, to in ((2, Zp2), (6, Zm2), (1, Zp1), (5, Zm1)):
            send(src, src, slz, lz.at[i - 1], to)
        left_out(0)

    def left_z(i):
        src = lpiece(z_of(i), x)
        arrived(src, lz.at[i - 1])
        if i == 2:
            send(src, src, slz, lz.at[2], Zp1)
            send(src, src, slz, lz.at[3], Zp2)
        if i == 6:
            send(src, src, slz, lz.at[6], Zm1)
        left_out(i)

    def left_x(which, i):
        x_, sem, j = {"p": (xm, lxp, 1), "m": (xp, lxm, 2), "2": (xo, lx2, 3)}[which]
        src = lpiece(z_of(i), x_)
        arrived(src, sem.at[i])
        if which == "p" and i % 2 == 0:
            send(src, src, slx, lx2.at[i], Xp)
        if which == "m" and i % 2 == 1:
            send(src, src, slx, lx2.at[i], Xm)
        send(src, src, sls, dl.at[j], Sib)

    def pick_right():
        loads[2].wait()
        v = rows_of(oldr, ids)
        rrow = pl.multiple_of(((zh * 2 + core) * 4 + y) * 32, 32)
        for b in range(8):
            h_, y_ = b % 2, b // 2
            rall[pl.ds(rrow, 32), h_ * 512 + y_ * 128:h_ * 512 + (y_ + 1) * 128] = v[:, b * 128:(b + 1) * 128]

    def build_new():
        nl[448:512, :] = jnp.zeros((64, SLAB), BF16)
        for h_ in range(2):
            nr[h_, 448:512, :] = jnp.zeros((64, 512), BF16)
        loads[3].wait()
        loads[4].wait()

        def body(i, _):
            at = pl.ds(pl.multiple_of(i * 32, 32), 32)
            nl[at, :] = rows_of(newl, [i * 8 + j for j in range(8)])
            v = rows_of(newr, [i * 8 + j for j in range(8)])
            for b in range(8):
                nr[b % 2, at, (b // 2) * 128:(b // 2 + 1) * 128] = v[:, b * 128:(b + 1) * 128]
            return 0

        lax.fori_loop(0, MEM // 8, body, 0)

    def own_member(n):
        r = lax.broadcasted_iota(jnp.int32, (n, 128), 0)
        c = lax.broadcasted_iota(jnp.int32, (n, 128), 1)
        return (r >> 3) == (c >> 2)

    def proj_part():
        loads[5].wait()
        lanes = pl.ds(pl.multiple_of(col * SLAB, SLAB), SLAB)
        for g in range(4):
            n = 256 if g < 3 else 128
            part = nt(tok[256 * g:256 * g + n, lanes], nl[128 * g:128 * (g + 1), :])
            part = jnp.where(own_member(n), part, 0.0)
            cx[x, :, 128 * g:128 * (g + 1)] = part.reshape(n // 8, 8, 128).sum(axis=0)
        src = cx.at[x]
        for to in (Xp, Xm, Xo):
            send(src, src, spx.at[0], px.at[0], to)

    def proj_x():
        arrived(cx.at[0:3], px.at[0])
        cz[zlo] = (cx[0] + cx[1]) + (cx[2] + cx[3])
        src = cz.at[zlo]
        for to in Zl:
            send(src, src, spx.at[1], px.at[1], to)

    def proj_z():
        arrived(cz.at[0:3], px.at[1])
        proj = ((cz[0] + cz[1]) + (cz[2] + cz[3])).astype(BF16).astype(F32)
        for g in range(4):
            n = 256 if g < 3 else 128
            wide = jnp.broadcast_to(proj[:, 128 * g:128 * (g + 1)][None], (n // 8, 8, 128)).reshape(n, 128)
            wide = jnp.where(own_member(n), wide, 0.0).astype(BF16)
            for h_ in range(2):
                acc[h_, 256 * g:256 * g + n, :] = nn(wide, nr[h_, 128 * g:128 * (g + 1), :]) * SIDE

    def main_dot(s, *ks):
        h_ = zh if s == 0 else 1 - zh
        deep = slice(ks[0] * LEN, (ks[-1] + 1) * LEN)
        arrived(wall.at[h_, 0:256, deep], dd.at[batch(s, ks[0])])
        for n in range(2):
            at = slice(n * 256, (n + 1) * 256)
            acc[h_, :, at] += nt(tok[:, deep], wall[h_, at, deep])

    xs = (x, xm, xp, xo)

    def slab(c):
        return pl.ds(pl.multiple_of(c * SLAB, SLAB), SLAB)

    def t_dot(j):
        cs = [zlo_ * 4 + xs[j] for zlo_ in range(4)]
        arrived(lall.at[0:2], dl.at[j])
        part = sum(nt(tok[:, slab(c)], lall[c]) for c in cs)
        tacc[...] = part if j == 0 else tacc[...] + part

    def make_rt():
        base = pl.multiple_of(zh * 512 + y * 128, 128)
        rt[...] = rall[:, pl.ds(base, 128)].astype(F32).T.astype(BF16)

    def update(j):
        left = rt[pl.ds(pl.multiple_of(core * OWN, OWN), OWN), :]
        for c in [zlo_ * 4 + xs[j] for zlo_ in range(4)]:
            own = wall[zh, pl.ds(pl.multiple_of((y * 2 + core) * OWN, OWN), OWN), slab(c)]
            upd[:, slab(c)] = (own.astype(F32) + nn(left, lall[c])).astype(BF16)

    def t_right(h_):
        if h_ == 0:
            tb[...] = tacc[...].astype(BF16)
        for n in range(2):
            at = slice(n * 256, (n + 1) * 256)
            acc[h_, :, at] += nn(tb[...], rall[:, h_ * 512 + n * 256:h_ * 512 + (n + 1) * 256])

    def finish(s):
        h_ = zh if s == 0 else 1 - zh
        for y_ in range(4):
            at = pl.ds(pl.multiple_of((2 * y_ + h_) * 128, 128), 128)
            pre = jnp.maximum(acc[h_, :, y_ * 128:(y_ + 1) * 128], 0.0)
            outv[:, at] = (pre * pre).astype(BF16)

    steps = {f.__name__: f for f in (
        start_left, own_y, own_z, pass_z, other_y, got_p, got_m, got_2, got_r, left_own, left_z, left_x,
        pick_right, build_new, proj_part, proj_x, proj_z, main_dot, t_dot, make_rt, update, t_right, finish,
    )}
    for name, *rest in ORDER:
        steps[name](*rest)

    for half in range(2):
        sent(wall.at[half], ssw.at[half])
    sent(wall.at[:, :, 0:LEN], ssw.at[2])
    sent(lall.at[0, 0:96, :], sly)
    sent(wall.at[0, 0:448, 0:LEN], slz)
    sent(lall.at[0:6], slx)
    sent(lall.at[0:8], sls)
    for j in range(2):
        sent(cx.at[0:3], spx.at[j])


def write_out(upd, act, upd_h, act_h, sem):
    copies = [pltpu.make_async_copy(act, act_h, sem.at[0]), pltpu.make_async_copy(upd, upd_h, sem.at[1])]
    for copy in copies:
        copy.start()
    for copy in copies:
        copy.wait()


def local(tokens, weight, old_left, old_right, selected, shaping, new_left, new_right):
    dma = pltpu.SemaphoreType.DMA
    anywhere = pl.BlockSpec(memory_space=pl.ANY)
    scalars = pl.BlockSpec(memory_space=pltpu.SMEM)
    upd, act = pl.pallas_call(
        kernel,
        out_shape=(pltpu.VMEM((OWN, D), BF16), pltpu.VMEM((ROWS, COLS), BF16)),
        in_specs=[anywhere] * 4 + [scalars] * 2 + [anywhere] * 2,
        out_specs=(pl.BlockSpec(memory_space=pltpu.VMEM),) * 2,
        scratch_shapes=[
            pltpu.VMEM((ROWS, D), BF16),
            pltpu.VMEM((2, 512, D), BF16),
            pltpu.VMEM((512, COLS), BF16),
            pltpu.VMEM((16, 512, SLAB), BF16),
            pltpu.VMEM((CHUNKS, OWN, LEN), BF16),
            pltpu.VMEM((32, COLS), BF16),
            pltpu.VMEM((MEM, RANK, SLAB), BF16),
            pltpu.VMEM((MEM, RANK, COLS), BF16),
            pltpu.VMEM((MEM, RANK, SLAB), BF16),
            pltpu.VMEM((MEM, RANK, COLS), BF16),
            pltpu.VMEM((512, SLAB), BF16),
            pltpu.VMEM((2, 512, 512), BF16),
            pltpu.VMEM((2, ROWS, 512), F32),
            pltpu.VMEM((ROWS, 512), F32),
            pltpu.VMEM((ROWS, 512), BF16),
            pltpu.VMEM((4, 8, 512), F32),
            pltpu.VMEM((4, 8, 512), F32),
            pltpu.VMEM((128, 512), BF16),
            dma((6,)), dma((3,)), dma(()), dma(()), dma(()), dma(()), dma((2,)),
            dma((2, NCH)), dma((2, NCH)), dma((2, NCH)), dma((NCH,)), dma((NCH,)), dma((11,)),
            dma(()), dma((7,)), dma((8,)), dma((8,)), dma((8,)), dma((4,)), dma((2,)),
        ],
        compiler_params=pltpu.CompilerParams(
            collective_id=0, has_side_effects=True, vmem_limit_bytes=56 * 1024 * 1024
        ),
        name="gather_and_project",
    )(tokens, weight.T, old_left, old_right, selected, shaping, new_left, new_right)
    upd, act = pl.pallas_call(
        write_out,
        out_shape=(
            jax.ShapeDtypeStruct((OWN, D), BF16),
            jax.ShapeDtypeStruct((ROWS, COLS), BF16),
        ),
        in_specs=[pl.BlockSpec(memory_space=pltpu.VMEM)] * 2,
        out_specs=(anywhere, anywhere),
        scratch_shapes=[dma((2,))],
        compiler_params=pltpu.CompilerParams(vmem_limit_bytes=8 * 1024 * 1024),
        name="write_out",
    )(upd, act)
    return (upd.T, act)


def solution(mesh):
    placed = (
        P("pop", None),
        P(None, ("col", "pop")),
        P("pop", None, "col"),
        P("pop", None, "col"),
        P("pop", None),
        P("pop", None),
        P("pop", None, "col"),
        P("pop", None, "col"),
    )
    return jax.shard_map(
        local,
        mesh=mesh,
        in_specs=placed,
        out_specs=(P(None, ("col", "pop")), P("pop", "col")),
        check_vma=False,
    )
```

```python
import functools
import math

import jax
import jax.numpy as jnp
from jax import lax
from jax.experimental import pallas as pl
from jax.experimental.pallas import tpu as pltpu
from jax.sharding import PartitionSpec as P

MESH = pl.DeviceIdType.MESH
F32, BF16 = jnp.float32, jnp.bfloat16

D = 4096
RANK = 4
ROWS = 896
COLS = 1024
OWN = 64
MEM = 112
SEL = 8
SLAB = 256
CHUNKS = 8
LEN = D // CHUNKS
RCH = CHUNKS
NCH = CHUNKS + 1
noise_scale = 0.5
ORDER = (
    ("start_left",), ("own_y", 0), ("own_z", 0), ("own_y", 1), ("own_z", 1), ("own_y", 2), ("own_y", 3),
    ("pick_right",), ("own_y", 8), ("own_y", 4), ("build_new",), ("proj_part",), ("own_z", 2), ("own_z", 3),
    ("own_y", 5), ("own_z", 8), ("own_z", 4), ("own_y", 6), ("own_z", 5), ("own_z", 6), ("own_y", 7), ("pass_z", 0),
    ("left_own",), ("got_m", 0, 0), ("proj_x",), ("got_p", 0, 0), ("got_m", 0, 1), ("got_p", 0, 1), ("got_m", 0, 2),
    ("got_p", 0, 2), ("pass_z", 1), ("got_m", 0, 3), ("got_p", 0, 3), ("left_x", "m", 0), ("left_x", "p", 0),
    ("got_m", 0, 8), ("got_p", 0, 8), ("got_m", 0, 4), ("got_p", 0, 4), ("left_z", 6), ("pass_z", 2), ("left_z", 5),
    ("got_m", 0, 5), ("got_p", 0, 5), ("pass_z", 3), ("other_y", 0), ("got_m", 0, 6), ("left_x", "2", 0),
    ("got_p", 0, 6), ("got_m", 0, 7), ("got_p", 0, 7), ("left_z", 2), ("left_z", 1), ("left_x", "m", 6),
    ("left_x", "p", 6), ("got_2", 0, 1), ("got_2", 0, 0), ("pass_z", 8), ("left_x", "m", 5), ("left_x", "p", 5),
    ("got_2", 0, 3), ("left_z", 7), ("got_2", 0, 2), ("other_y", 1), ("got_2", 0, 8), ("proj_z",), ("got_2", 0, 4),
    ("pass_z", 4), ("main_dot", 0, 0, 1), ("got_2", 0, 5), ("left_x", "m", 2), ("left_x", "p", 2), ("got_p", 1, 0),
    ("main_dot", 0, 2, 3), ("left_z", 3), ("left_x", "m", 1), ("own_z", 7), ("left_x", "p", 1), ("got_m", 1, 0),
    ("got_2", 0, 6), ("other_y", 2), ("got_r", 0), ("pass_z", 5), ("left_x", "2", 5), ("left_x", "2", 6),
    ("got_2", 0, 7), ("got_p", 1, 1), ("other_y", 3), ("main_dot", 0, 4, 5), ("left_x", "m", 7), ("left_x", "p", 7),
    ("got_m", 1, 1), ("pass_z", 6), ("left_z", 4), ("left_x", "2", 2), ("got_2", 1, 0), ("main_dot", 0, 6, 7),
    ("left_x", "m", 3), ("got_m", 1, 2), ("left_x", "p", 3), ("got_p", 1, 2), ("pass_z", 7), ("other_y", 8),
    ("t_dot", 0), ("left_x", "2", 1), ("got_m", 1, 3), ("got_p", 1, 3), ("left_x", "2", 7), ("got_2", 1, 1),
    ("other_y", 4), ("left_x", "p", 4), ("left_x", "m", 4), ("got_2", 1, 2), ("left_x", "2", 3), ("got_m", 1, 8),
    ("main_dot", 1, 0, 1), ("other_y", 5), ("got_p", 1, 8), ("t_dot", 1), ("other_y", 6), ("got_2", 1, 3),
    ("t_dot", 2), ("left_x", "2", 4), ("got_m", 1, 4), ("got_p", 1, 4), ("other_y", 7), ("got_2", 1, 8),
    ("main_dot", 1, 2, 3), ("got_p", 1, 5), ("t_dot", 3), ("got_m", 1, 5), ("got_p", 1, 6), ("got_m", 1, 6),
    ("got_r", 1), ("make_rt",), ("t_right", 0), ("t_right", 1), ("got_2", 1, 4), ("update", 0), ("update", 1),
    ("got_m", 1, 7), ("update", 2), ("update", 3), ("got_p", 1, 7), ("finish", 0), ("got_2", 1, 5), ("got_2", 1, 6),
    ("main_dot", 1, 4, 5), ("got_2", 1, 7), ("main_dot", 1, 6), ("last_dot", 7),
)
FACTOR = 1.0 / math.sqrt(D * RANK * SEL * 16)
SIDE = noise_scale / math.sqrt(D * RANK)


def batch(s, k):
    if s == 0:
        return k // 2
    return 5 + (k // 2 if k < 6 else k - 3)


def going_up(k):
    return k % 2 == 0 and k != RCH


def nt(a, b):
    return lax.dot_general(a, b, (((1,), (1,)), ((), ())), preferred_element_type=F32)


def nn(a, b):
    return lax.dot_general(a, b, (((1,), (0,)), ((), ())), preferred_element_type=F32)


def kernel(
    tok_h, w_h, oldl_h, oldr_h, sel, shp, newl_h, newr_h,
    upd, outv,
    tok, wall, rall, lall, trw, trr, oldl, oldr, newl, newr, nl, nr,
    acc, tacc, tb, cx, cz, rt,
    ld, ssw, sly, slz, slx, sls, spx,
    rp, rm, r2, tz, rz, dd, ly, lz, lxp, lxm, lx2, dl, px,
):
    pop, col = lax.axis_index("pop"), lax.axis_index("col")
    y, zh, core = pop // 4, (pop // 2) % 2, pop % 2
    zlo, x = col // 4, col % 4
    z = zh * 4 + zlo

    def dev(y_, z_, core_, x_):
        return (y_ * 4 + (z_ // 4) * 2 + core_, (z_ % 4) * 4 + x_)

    yp, ym, yo = (y + 1) % 4, (y + 3) % 4, (y + 2) % 4
    xp, xm, xo = (x + 1) % 4, (x + 3) % 4, (x + 2) % 4
    Yp, Ym, Yo = dev(yp, z, core, x), dev(ym, z, core, x), dev(yo, z, core, x)
    Xp, Xm, Xo = dev(y, z, core, xp), dev(y, z, core, xm), dev(y, z, core, xo)

    def zdev(step):
        return dev(y, (z + step + 8) % 8, core, x)

    Zp1, Zm1, Zp2, Zm2, Zp3, Zm3 = [zdev(step) for step in (1, -1, 2, -2, 3, -3)]
    Sib = dev(y, z, 1 - core, x)
    Zl = [dev(y, zh * 4 + (zlo + j) % 4, core, x) for j in (1, 2, 3)]

    def send(src, dst, ssem, rsem, to):
        pltpu.make_async_remote_copy(
            src_ref=src, dst_ref=dst, send_sem=ssem, recv_sem=rsem,
            device_id=to, device_id_type=MESH,
        ).start()

    def arrived(dst, rsem):
        pltpu.make_async_remote_copy(
            src_ref=dst, dst_ref=dst, send_sem=ssw.at[0], recv_sem=rsem,
            device_id=Sib, device_id_type=MESH,
        ).wait_recv()

    def sent(src, ssem):
        pltpu.make_async_remote_copy(
            src_ref=src, dst_ref=src, send_sem=ssem, recv_sem=rp.at[0, 0],
            device_id=Sib, device_id_type=MESH,
        ).wait_send()

    def piece(zh_, y_, k):
        if k == RCH:
            return rall.at[pl.ds(pl.multiple_of(((zh_ * 2 + core) * 4 + y_) * 32, 32), 32), :]
        return wall.at[zh_, pl.ds(pl.multiple_of((y_ * 2 + core) * OWN, OWN), OWN), k * LEN:(k + 1) * LEN]

    def transit(k):
        return trr if k == RCH else trw.at[k]

    def lpiece(z_, x_):
        c_ = (z_ % 4) * 4 + x_
        return lall.at[c_, pl.ds(pl.multiple_of(((z_ // 4) * 2 + core) * 128, 128), 128), :]

    mine = wall.at[zh, pl.ds(pl.multiple_of((y * 2 + core) * OWN, OWN), OWN), :]
    loads = [
        pltpu.make_async_copy(s, d, ld.at[i])
        for i, (s, d) in enumerate((
            (w_h, mine), (oldl_h, oldl), (oldr_h, oldr), (newl_h, newl), (newr_h, newr), (tok_h, tok),
        ))
    ]
    for i in (1, 0, 2, 5, 3, 4):
        loads[i].start()

    barrier = pltpu.get_barrier_semaphore()
    partners = [Yp, Ym, Yo, Xp, Xm, Xo, Zp1, Zm1, Zp2, Zm2, Zp3, Zm3, Sib] + Zl
    for to in partners:
        pl.semaphore_signal(barrier, inc=1, device_id=to, device_id_type=MESH)

    def rows_of(ref, ids, scales=None):
        parts = [ref[i].astype(F32) for i in ids]
        if scales is not None:
            parts = [p * s for p, s in zip(parts, scales)]
        return jnp.concatenate(parts, axis=0).astype(BF16)

    ids = [sel[0, j] for j in range(SEL)]
    loads[1].wait()
    lrow = pl.multiple_of((zh * 2 + core) * 128 + y * 32, 32)
    lall[col, pl.ds(lrow, 32), :] = rows_of(oldl, ids, [shp[0, j] * F32(FACTOR) for j in range(SEL)])
    loads[0].wait()
    pl.semaphore_wait(barrier, len(partners))

    def start_left():
        src = lall.at[col, pl.ds(lrow, 32), :]
        for j, to in enumerate((Yp, Ym, Yo)):
            send(src, src, sly, ly, to)

    def own_y(k):
        src = piece(zh, y, k)
        send(src, src, ssw.at[k // 4], rp.at[0, k], Yp)
        send(src, src, ssw.at[k // 4], rm.at[0, k], Ym)
        send(src, src, ssw.at[k // 4], dd.at[batch(0, k)], Sib)

    def own_z(k):
        send(piece(zh, y, k), transit(k), ssw.at[k // 4], tz.at[k], Zp1 if going_up(k) else Zm1)

    def pass_z(k):
        arrived(transit(k), tz.at[k])
        from_zh = ((z + (7 if going_up(k) else 1)) % 8) // 4
        send(transit(k), piece(from_zh, y, k), ssw.at[k // 4], rz.at[k], Zp3 if going_up(k) else Zm3)

    def other_y(k):
        src = piece(1 - zh, y, k)
        arrived(src, rz.at[k])
        send(src, src, ssw.at[k // 4], rp.at[1, k], Yp)
        send(src, src, ssw.at[k // 4], rm.at[1, k], Ym)
        send(src, src, ssw.at[k // 4], dd.at[batch(1, k)], Sib)

    def got_p(s, k):
        h_ = zh if s == 0 else 1 - zh
        src = piece(h_, ym, k)
        arrived(src, rp.at[s, k])
        if going_up(k):
            send(src, src, ssw.at[k // 4], r2.at[s, k], Yp)
        send(src, src, ssw.at[k // 4], dd.at[batch(s, k)], Sib)

    def got_m(s, k):
        h_ = zh if s == 0 else 1 - zh
        src = piece(h_, yp, k)
        arrived(src, rm.at[s, k])
        if not going_up(k):
            send(src, src, ssw.at[k // 4], r2.at[s, k], Ym)
        send(src, src, ssw.at[k // 4], dd.at[batch(s, k)], Sib)

    def got_2(s, k):
        h_ = zh if s == 0 else 1 - zh
        src = piece(h_, yo, k)
        arrived(src, r2.at[s, k])
        send(src, src, ssw.at[k // 4], dd.at[batch(s, k)], Sib)

    def got_r(s):
        arrived(rall.at[0:128, :], dd.at[batch(s, RCH)])

    def z_of(i):
        return z if i == 0 else ((z + 8 - i) % 8 if i <= 4 else (z + i - 4) % 8)

    def left_out(i):
        src = lpiece(z_of(i), x)
        send(src, src, slx, lxp.at[i], Xp)
        send(src, src, slx, lxm.at[i], Xm)
        send(src, src, sls, dl.at[0], Sib)

    def left_own():
        arrived(lall.at[0, 0:96, :], ly)
        src = lpiece(z, x)
        for i, to in ((2, Zp2), (6, Zm2), (1, Zp1), (5, Zm1)):
            send(src, src, slz, lz.at[i - 1], to)
        left_out(0)

    def left_z(i):
        src = lpiece(z_of(i), x)
        arrived(src, lz.at[i - 1])
        if i == 2:
            send(src, src, slz, lz.at[2], Zp1)
            send(src, src, slz, lz.at[3], Zp2)
        if i == 6:
            send(src, src, slz, lz.at[6], Zm1)
        left_out(i)

    def left_x(which, i):
        x_, sem, j = {"p": (xm, lxp, 1), "m": (xp, lxm, 2), "2": (xo, lx2, 3)}[which]
        src = lpiece(z_of(i), x_)
        arrived(src, sem.at[i])
        if which == "p" and i % 2 == 0:
            send(src, src, slx, lx2.at[i], Xp)
        if which == "m" and i % 2 == 1:
            send(src, src, slx, lx2.at[i], Xm)
        send(src, src, sls, dl.at[j], Sib)

    def pick_right():
        loads[2].wait()
        v = rows_of(oldr, ids)
        rrow = pl.multiple_of(((zh * 2 + core) * 4 + y) * 32, 32)
        for b in range(8):
            h_, y_ = b % 2, b // 2
            rall[pl.ds(rrow, 32), h_ * 512 + y_ * 128:h_ * 512 + (y_ + 1) * 128] = v[:, b * 128:(b + 1) * 128]

    def build_new():
        nl[448:512, :] = jnp.zeros((64, SLAB), BF16)
        for h_ in range(2):
            nr[h_, 448:512, :] = jnp.zeros((64, 512), BF16)
        loads[3].wait()
        loads[4].wait()

        def body(i, _):
            at = pl.ds(pl.multiple_of(i * 32, 32), 32)
            nl[at, :] = rows_of(newl, [i * 8 + j for j in range(8)])
            v = rows_of(newr, [i * 8 + j for j in range(8)])
            for b in range(8):
                nr[b % 2, at, (b // 2) * 128:(b // 2 + 1) * 128] = v[:, b * 128:(b + 1) * 128]
            return 0

        lax.fori_loop(0, MEM // 8, body, 0)

    def own_member(n):
        r = lax.broadcasted_iota(jnp.int32, (n, 128), 0)
        c = lax.broadcasted_iota(jnp.int32, (n, 128), 1)
        return (r >> 3) == (c >> 2)

    def proj_part():
        loads[5].wait()
        lanes = pl.ds(pl.multiple_of(col * SLAB, SLAB), SLAB)
        for g in range(4):
            n = 256 if g < 3 else 128
            part = nt(tok[256 * g:256 * g + n, lanes], nl[128 * g:128 * (g + 1), :])
            part = jnp.where(own_member(n), part, 0.0)
            cx[x, :, 128 * g:128 * (g + 1)] = part.reshape(n // 8, 8, 128).sum(axis=0)
        src = cx.at[x]
        for to in (Xp, Xm, Xo):
            send(src, src, spx.at[0], px.at[0], to)

    def proj_x():
        arrived(cx.at[0:3], px.at[0])
        cz[zlo] = (cx[0] + cx[1]) + (cx[2] + cx[3])
        src = cz.at[zlo]
        for to in Zl:
            send(src, src, spx.at[1], px.at[1], to)

    def proj_z():
        arrived(cz.at[0:3], px.at[1])
        proj = ((cz[0] + cz[1]) + (cz[2] + cz[3])).astype(BF16).astype(F32)
        for g in range(4):
            n = 256 if g < 3 else 128
            wide = jnp.broadcast_to(proj[:, 128 * g:128 * (g + 1)][None], (n // 8, 8, 128)).reshape(n, 128)
            wide = jnp.where(own_member(n), wide, 0.0).astype(BF16)
            for h_ in range(2):
                acc[h_, 256 * g:256 * g + n, :] = nn(wide, nr[h_, 128 * g:128 * (g + 1), :]) * SIDE

    def main_dot(s, *ks):
        h_ = zh if s == 0 else 1 - zh
        deep = slice(ks[0] * LEN, (ks[-1] + 1) * LEN)
        arrived(wall.at[h_, 0:256, deep], dd.at[batch(s, ks[0])])
        for n in range(2):
            at = slice(n * 256, (n + 1) * 256)
            acc[h_, :, at] += nt(tok[:, deep], wall[h_, at, deep])

    xs = (x, xm, xp, xo)

    def slab(c):
        return pl.ds(pl.multiple_of(c * SLAB, SLAB), SLAB)

    def t_dot(j):
        cs = [zlo_ * 4 + xs[j] for zlo_ in range(4)]
        arrived(lall.at[0:2], dl.at[j])
        part = sum(nt(tok[:, slab(c)], lall[c]) for c in cs)
        tacc[...] = part if j == 0 else tacc[...] + part

    def make_rt():
        base = pl.multiple_of(zh * 512 + y * 128, 128)
        rt[...] = rall[:, pl.ds(base, 128)].astype(F32).T.astype(BF16)

    def update(j):
        left = rt[pl.ds(pl.multiple_of(core * OWN, OWN), OWN), :]
        for c in [zlo_ * 4 + xs[j] for zlo_ in range(4)]:
            own = wall[zh, pl.ds(pl.multiple_of((y * 2 + core) * OWN, OWN), OWN), slab(c)]
            upd[:, slab(c)] = (own.astype(F32) + nn(left, lall[c])).astype(BF16)

    def t_right(h_):
        if h_ == 0:
            tb[...] = tacc[...].astype(BF16)
        for n in range(2):
            at = slice(n * 256, (n + 1) * 256)
            acc[h_, :, at] += nn(tb[...], rall[:, h_ * 512 + n * 256:h_ * 512 + (n + 1) * 256])

    def put(h_, y_, pre):
        at = pl.ds(pl.multiple_of((2 * y_ + h_) * 128, 128), 128)
        pre = jnp.maximum(pre, 0.0)
        outv[:, at] = (pre * pre).astype(BF16)

    def finish(s):
        h_ = zh if s == 0 else 1 - zh
        for y_ in range(4):
            put(h_, y_, acc[h_, :, y_ * 128:(y_ + 1) * 128])

    def last_dot(k):
        h_, deep = 1 - zh, slice(k * LEN, (k + 1) * LEN)
        arrived(wall.at[h_, 0:256, deep], dd.at[batch(1, k)])
        for n in range(2):
            at = slice(n * 256, (n + 1) * 256)
            pre = acc[h_, :, at] + nt(tok[:, deep], wall[h_, at, deep])
            for j in range(2):
                put(h_, 2 * n + j, pre[:, j * 128:(j + 1) * 128])

    steps = {f.__name__: f for f in (
        start_left, own_y, own_z, pass_z, other_y, got_p, got_m, got_2, got_r, left_own, left_z, left_x,
        pick_right, build_new, proj_part, proj_x, proj_z, main_dot, t_dot, make_rt, update, t_right, finish, last_dot,
    )}
    for name, *rest in ORDER:
        steps[name](*rest)

    for half in range(2):
        sent(wall.at[half], ssw.at[half])
    sent(wall.at[:, :, 0:LEN], ssw.at[2])
    sent(lall.at[0, 0:96, :], sly)
    sent(wall.at[0, 0:448, 0:LEN], slz)
    sent(lall.at[0:6], slx)
    sent(lall.at[0:8], sls)
    for j in range(2):
        sent(cx.at[0:3], spx.at[j])


def write_out(upd, act, upd_h, act_h, sem):
    copies = [pltpu.make_async_copy(act, act_h, sem.at[0]), pltpu.make_async_copy(upd, upd_h, sem.at[1])]
    for copy in copies:
        copy.start()
    for copy in copies:
        copy.wait()


def local(tokens, weight, old_left, old_right, selected, shaping, new_left, new_right):
    dma = pltpu.SemaphoreType.DMA
    anywhere = pl.BlockSpec(memory_space=pl.ANY)
    scalars = pl.BlockSpec(memory_space=pltpu.SMEM)
    upd, act = pl.pallas_call(
        kernel,
        out_shape=(pltpu.VMEM((OWN, D), BF16), pltpu.VMEM((ROWS, COLS), BF16)),
        in_specs=[anywhere] * 4 + [scalars] * 2 + [anywhere] * 2,
        out_specs=(pl.BlockSpec(memory_space=pltpu.VMEM),) * 2,
        scratch_shapes=[
            pltpu.VMEM((ROWS, D), BF16),
            pltpu.VMEM((2, 512, D), BF16),
            pltpu.VMEM((512, COLS), BF16),
            pltpu.VMEM((16, 512, SLAB), BF16),
            pltpu.VMEM((CHUNKS, OWN, LEN), BF16),
            pltpu.VMEM((32, COLS), BF16),
            pltpu.VMEM((MEM, RANK, SLAB), BF16),
            pltpu.VMEM((MEM, RANK, COLS), BF16),
            pltpu.VMEM((MEM, RANK, SLAB), BF16),
            pltpu.VMEM((MEM, RANK, COLS), BF16),
            pltpu.VMEM((512, SLAB), BF16),
            pltpu.VMEM((2, 512, 512), BF16),
            pltpu.VMEM((2, ROWS, 512), F32),
            pltpu.VMEM((ROWS, 512), F32),
            pltpu.VMEM((ROWS, 512), BF16),
            pltpu.VMEM((4, 8, 512), F32),
            pltpu.VMEM((4, 8, 512), F32),
            pltpu.VMEM((128, 512), BF16),
            dma((6,)), dma((3,)), dma(()), dma(()), dma(()), dma(()), dma((2,)),
            dma((2, NCH)), dma((2, NCH)), dma((2, NCH)), dma((NCH,)), dma((NCH,)), dma((11,)),
            dma(()), dma((7,)), dma((8,)), dma((8,)), dma((8,)), dma((4,)), dma((2,)),
        ],
        compiler_params=pltpu.CompilerParams(
            collective_id=0, has_side_effects=True, vmem_limit_bytes=56 * 1024 * 1024
        ),
        name="gather_and_project",
    )(tokens, weight.T, old_left, old_right, selected, shaping, new_left, new_right)
    upd, act = pl.pallas_call(
        write_out,
        out_shape=(
            jax.ShapeDtypeStruct((OWN, D), BF16),
            jax.ShapeDtypeStruct((ROWS, COLS), BF16),
        ),
        in_specs=[pl.BlockSpec(memory_space=pltpu.VMEM)] * 2,
        out_specs=(anywhere, anywhere),
        scratch_shapes=[dma((2,))],
        compiler_params=pltpu.CompilerParams(vmem_limit_bytes=8 * 1024 * 1024),
        name="write_out",
    )(upd, act)
    return (upd.T, act)


def solution(mesh):
    placed = (
        P("pop", None),
        P(None, ("col", "pop")),
        P("pop", None, "col"),
        P("pop", None, "col"),
        P("pop", None),
        P("pop", None),
        P("pop", None, "col"),
        P("pop", None, "col"),
    )
    return jax.shard_map(
        local,
        mesh=mesh,
        in_specs=placed,
        out_specs=(P(None, ("col", "pop")), P("pop", "col")),
        check_vma=False,
    )
```
